32 devices in a mesh: seq: 8 (over z, y), batch: 4 (over x, core).
Axes of the slice: x: 2, y: 2, z: 4, core: 2. Of those that a mesh axis runs over, the one named last changes fastest.
Arguments:
- tokens: bfloat16 [4096, 1440], P(('batch', 'seq')), parts along dimension 0, may hold values from -6 to 6
- norm_gain: float32 [1440], replicated, may hold values from 0.1 to 1.9
- qkv_weight: bfloat16 [1440, 2560], P(None, 'seq'), may hold values from -2 to 2
- sinks: float32 [32], replicated, may hold values from 0 to 5
- out_weight: bfloat16 [2048, 1440], P('seq'), may hold values from -0.125 to 0.125
- moe_gain: float32 [1440], replicated, may hold values from 0.1 to 1.9
- expert_in: bfloat16 [8, 1440, 2880], P('seq'), may hold values from -0.15625 to 0.15625
- expert_out: bfloat16 [8, 1440, 1440], P('seq'), may hold values from -0.15625 to 0.15625
- expert_ids: int32 [4096, 4], P(('batch', 'seq')), parts along dimension 0, may hold values from 0 to 7, all different within a row; in each aligned block of 128 rows (0 to 127, 128 to 255, ...) at most 128 rows name the same one
- gate_ints: int32 [4096, 4], P(('batch', 'seq')), parts along dimension 0, may hold values from 1 to 4096
Outputs:
- block_out: bfloat16 [4096, 1440], P(('batch', 'seq')), parts along dimension 0
The draws below stay inside these ranges and needn't reach their ends.
There are 4 independent parts, one for each index of `batch`. The reference program is written for one: setup_inputs(seed, part) draws one part's arguments, and reference() takes and returns one part's arrays. A program takes and returns all parts, laid end to end along the dimension named above; an argument that names none is the same for every part. Nothing has to cross between parts.
Inputs may be any that keep to these rules, and one draw needn't show every extreme that they name: `expert_ids`: each row names 4 different experts; among the 128 rows of one device no expert is named more than 128 times.
All inputs are finite; a program needn't handle non-finite values.
Results may differ from the reference program's by a relative error of at most 0.012.
Values may be sent and summed in bfloat16 or wider, within the bound.
A program may use at most 128 MiB of HBM per device.

```python
import math
import jax
import jax.numpy as jnp
import numpy as np
from jax import lax

D = 1440
H = 1440
QH = 32
KVH = 4
HD = 64
WIN = 128
TOP = 4
TOK_DEV = 128
EXPERTS = 8
CAP = 128
SEQ_LEN = 1024
N_SEQ = 8


def draw_qkv_weight(key, part):
    columns = (QH + 2 * KVH) * HD
    normal_part = jax.random.truncated_normal(key, -4.0, 4.0, (D, columns), jnp.float32) * D ** (-0.5)
    return jnp.clip(normal_part, -2.0, 2.0).astype(jnp.bfloat16)


def place_ends(array, stream_key, least, top_value):
    longest = array.shape.index(max(array.shape))
    spots = []
    for shift in (0, 1):
        where = [jax.random.randint(jax.random.fold_in(stream_key, axis), (), 0, length) for axis, length in enumerate(array.shape)]
        where[longest] = (where[longest] + shift) % array.shape[longest]
        spots.append(tuple(where))
    return array.at[spots[0]].set(least).at[spots[1]].set(top_value)


def block_levels(key, shape, shards, least, top_value):
    factor_of = 1.0
    for position, parts in shards:
        steps = jax.random.uniform(jax.random.fold_in(jax.random.fold_in(key, 6), position), (parts,), jnp.float32, least / len(shards), top_value / len(shards))
        factor_of = factor_of * jnp.repeat(jnp.exp(steps), shape[position] // parts).reshape((-1,) + (1,) * (len(shape) - 1 - position))
    return factor_of


def routed_block(own_key, own, number, rows, count, top, most, lean):
    order = jax.random.permutation(own_key, count)
    packed, usual = load_shares(count, rows * top, most, lean, True), load_shares(count, rows * top, most, lean, False)
    places = jnp.arange(count)

    def named(tallies, offset_by):
        used = int((tallies > 0).sum())
        fixed = max(1, used // 4)
        shifted = fixed + (places - fixed + offset_by * (used - fixed)) % max(1, count - fixed)
        return jnp.zeros((count,), jnp.int32).at[order[jnp.where(places < fixed, places, shifted)]].set(jnp.asarray(tallies, jnp.int32))

    tallies = jnp.where(number % 4 == 0, named(packed, number // 4), named(usual, number - number // 4 - 1))
    mixed = jax.random.permutation(jax.random.fold_in(own, 3), count)
    source_of, sink = mixed[0:count // 2 * 2:2], mixed[1:count // 2 * 2:2]
    slack = jnp.minimum(tallies[source_of] - 1, most - tallies[sink]) // 2
    slack = jnp.where((source_of == order[0]) | (sink == order[0]) | (tallies[sink] == 0), 0, jnp.maximum(slack, 0))
    shifted = jax.random.randint(jax.random.fold_in(own, 4), (count // 2,), 0, 1 << 20) % (slack + 1)
    tallies = tallies.at[source_of].add(-shifted).at[sink].add(shifted)
    members = jnp.searchsorted(jnp.cumsum(tallies), jnp.arange(rows * top), side="right").astype(jnp.int32)
    listing = members.reshape(top, rows).T
    listing = listing[jax.random.permutation(jax.random.fold_in(own, 1), rows)]
    offset_by = jax.random.randint(jax.random.fold_in(own, 2), (rows, 1), 0, top)
    return jnp.take_along_axis(listing, (jnp.arange(top)[None, :] + offset_by) % top, axis=1)


def load_shares(count, total, most, slope, full):
    loads = [(1 << 20) // math.isqrt(grade ** slope) + 1 for grade in range(1, count + 1)]
    largest = most if full else min(most, max(-(-total // count), total * loads[0] // sum(loads)))
    least = 1 if total - largest >= count - 1 else 0
    given, spare = [largest] + [least] * (count - 1), total - largest - least * (count - 1)
    while spare > 0:
        movable = [i for i in range(1, count) if given[i] < largest] or [i for i in range(1, count) if given[i] < most]
        mass, budget = sum([loads[i] for i in movable]), spare
        for i in movable:
            extra = min(most - given[i], max(1, budget * loads[i] // mass), spare)
            given[i] = given[i] + extra
            spare = spare - extra
    return np.array(given)


def normal_values(own_key, shape, deviation, limit, split=(), kind=jnp.bfloat16):
    entries = jax.random.normal(own_key, shape, jnp.float32) * deviation
    if len(split) > 0:
        entries = block_levels(own_key, shape, split, -0.22, 0.18) * entries
    return jnp.clip(entries, min=-limit, max=limit).astype(kind)


def setup_inputs(seed: int = 0, part: int = 0) -> dict:
    seeds = jax.random.split(jax.random.key(seed), 11)
    part_splits = jax.random.split(jax.random.fold_in(seeds[10], part), 11)
    tokens = normal_values(part_splits[0], (SEQ_LEN, D), 1.0, 6.0, ((0, 8),))
    norm_gain = jnp.clip(1.0 + 0.18 * jax.random.normal(seeds[1], (D,), jnp.float32), 0.1, 1.9)
    qkv_weight = draw_qkv_weight(jax.random.fold_in(seeds[10], 71), part)
    sinks = jnp.clip(jax.random.uniform(seeds[3], (QH,), jnp.float32, 0.0, 5.0), 0.0, 5.0)
    out_weight = normal_values(seeds[4], (QH * HD, D), (QH * HD) ** -0.5, 0.125, ((0, 8),))
    moe_gain = jnp.clip(1.0 + 0.18 * jax.random.normal(seeds[5], (D,), jnp.float32), 0.1, 1.9)
    expert_in = normal_values(seeds[6], (EXPERTS, D, 2 * H), D ** -0.5, 0.15625, ((0, 8),))
    expert_out = normal_values(seeds[7], (EXPERTS, H, D), H ** -0.5, 0.15625, ((0, 8),))
    expert_ids_keys = jax.random.split(jax.random.fold_in(part_splits[8], 1), SEQ_LEN // TOK_DEV)
    expert_ids_turns = jax.random.permutation(jax.random.fold_in(part_splits[8], 3), SEQ_LEN // TOK_DEV)
    expert_ids = jax.vmap(lambda own, number: routed_block(jax.random.fold_in(part_splits[8], 2), own, number, TOK_DEV, EXPERTS, TOP, CAP, 2))(expert_ids_keys, expert_ids_turns).reshape((SEQ_LEN, TOP))
    gate_ints = place_ends(jax.random.randint(part_splits[9], (SEQ_LEN, TOP), 1, 4097), jax.random.fold_in(part_splits[9], 1), 1, 4096).astype(jnp.int32)
    return dict(tokens=tokens, norm_gain=norm_gain, qkv_weight=qkv_weight, sinks=sinks, out_weight=out_weight, moe_gain=moe_gain, expert_in=expert_in, expert_out=expert_out, expert_ids=expert_ids, gate_ints=gate_ints)


epsilon = 1e-05
rope_base = 150000.0
glu_slope = 1.702

def norm_scale(values, gain):
    widened = values.astype(jnp.float32)
    mean_sq = lax.optimization_barrier(jnp.mean(widened * widened, axis=-1, keepdims=True))
    return widened * lax.rsqrt(mean_sq + epsilon) * gain.astype(jnp.float32)

def rotate(values, positions):
    half_width = values.shape[-1] // 2
    freq_steps = jnp.arange(half_width).astype(jnp.float32)
    inverse = jnp.exp(freq_steps * (-2.0 * math.log(rope_base) / values.shape[-1]))
    angles = positions[:, None] * inverse[None, :]
    cosine = jnp.cos(angles)[:, None, :]
    sine_term = jnp.sin(angles)[:, None, :]
    lower_half = values[..., :half_width]
    second = values[..., half_width:]
    return jnp.concatenate([lower_half * cosine - second * sine_term, second * cosine + lower_half * sine_term], axis=-1)

def band_block(queries, key_heads, value_heads, sinks, first_pos):
    count = queries.shape[0]
    groups = QH // KVH
    grouped = queries.reshape(count, KVH, groups, HD).astype(jnp.float32)
    scores = jnp.einsum('tkgd,skd->kgts', grouped, key_heads.astype(jnp.float32)) * (1.0 / math.sqrt(HD))
    query_pos = first_pos + jnp.arange(count).astype(jnp.int32)
    key_pos = first_pos - count + jnp.arange(2 * count).astype(jnp.int32)
    distance = query_pos[:, None] - key_pos[None, :]
    allowed = (distance >= 0) & (distance < WIN) & (key_pos >= 0)[None, :]
    scores = jnp.where(allowed[None, None, :, :], scores, -jnp.inf)
    sink_logit = sinks.reshape(KVH, groups, 1, 1).astype(jnp.float32)
    row_peak = jnp.maximum(lax.optimization_barrier(jnp.max(scores, axis=-1, keepdims=True)), sink_logit)
    raised = jnp.exp(scores - row_peak)
    totals = lax.optimization_barrier(jnp.sum(raised, axis=-1, keepdims=True)) + jnp.exp(sink_logit - row_peak)
    weights = (raised / totals).astype(jnp.bfloat16)
    mixture = jnp.einsum('kgts,skd->tkgd', weights.astype(jnp.float32), value_heads.astype(jnp.float32))
    return mixture.reshape(count, QH * HD).astype(jnp.bfloat16)

def reference(tokens, norm_gain, qkv_weight, sinks, out_weight, moe_gain, expert_in, expert_out, expert_ids, gate_ints):
    seq_len = tokens.shape[0]
    local_rows = TOK_DEV
    query_cols = QH * HD
    key_cols = KVH * HD
    residual = tokens.astype(jnp.float32)
    normed = norm_scale(tokens, norm_gain).astype(jnp.bfloat16)
    projections = jnp.dot(normed, qkv_weight, preferred_element_type=jnp.float32)
    positions = jnp.arange(seq_len).astype(jnp.float32)
    queries = rotate(projections[:, :query_cols].reshape(seq_len, QH, HD), positions).astype(jnp.bfloat16)
    key_heads = rotate(projections[:, query_cols:query_cols + key_cols].reshape(seq_len, KVH, HD), positions).astype(jnp.bfloat16)
    value_heads = projections[:, query_cols + key_cols:].reshape(seq_len, KVH, HD).astype(jnp.bfloat16)
    padding = jnp.zeros((local_rows, KVH, HD), jnp.bfloat16)
    prev_keys = jnp.concatenate([padding, key_heads[:seq_len - local_rows]], axis=0).reshape(N_SEQ, local_rows, KVH, HD)
    prev_values = jnp.concatenate([padding, value_heads[:seq_len - local_rows]], axis=0).reshape(N_SEQ, local_rows, KVH, HD)
    key_blocks = jnp.concatenate([prev_keys, key_heads.reshape(N_SEQ, local_rows, KVH, HD)], axis=1)
    value_blocks = jnp.concatenate([prev_values, value_heads.reshape(N_SEQ, local_rows, KVH, HD)], axis=1)
    query_blocks = queries.reshape(N_SEQ, local_rows, QH, HD)
    starts = (jnp.arange(N_SEQ) * local_rows).astype(jnp.int32)

    def attend(element):
        return band_block(element[0], element[1], element[2], sinks, element[3])
    attention = lax.map(attend, (query_blocks, key_blocks, value_blocks, starts)).reshape(seq_len, query_cols)
    projected = jnp.dot(attention, out_weight, preferred_element_type=jnp.float32)
    residual_mid = (residual + projected).astype(jnp.bfloat16)
    moe_input = norm_scale(residual_mid, moe_gain).astype(jnp.bfloat16)
    id_blocks = expert_ids.reshape(N_SEQ, local_rows * TOP)
    onehot = (id_blocks[:, :, None] == jnp.arange(EXPERTS).astype(jnp.int32)[None, None, :]).astype(jnp.int32)
    before = jnp.cumsum(onehot, axis=1) - onehot
    slot_index = lax.optimization_barrier(jnp.sum(before * onehot, axis=2))
    expert_rows = N_SEQ * CAP
    target = (id_blocks * expert_rows + jnp.arange(N_SEQ).astype(jnp.int32)[:, None] * CAP + slot_index).reshape(-1).astype(jnp.int32)
    source = jnp.repeat(moe_input, TOP, axis=0)
    buffer = jnp.zeros((EXPERTS * expert_rows, tokens.shape[1]), jnp.bfloat16).at[target].set(source)

    def expert(element):
        slab, weight_in, weight_out = element
        paired = jnp.dot(slab, weight_in, preferred_element_type=jnp.float32)
        gate_part = paired[:, :H]
        up_part = paired[:, H:]
        activated = (gate_part * jax.nn.sigmoid(glu_slope * gate_part) * (up_part + 1.0)).astype(jnp.bfloat16)
        return jnp.dot(activated, weight_out, preferred_element_type=jnp.float32).astype(jnp.bfloat16)
    results = lax.map(expert, (buffer.reshape(EXPERTS, expert_rows, tokens.shape[1]), expert_in, expert_out))
    picked = results.reshape(EXPERTS * expert_rows, tokens.shape[1])[target].reshape(seq_len, TOP, tokens.shape[1])
    route_weight = gate_ints.astype(jnp.float32)
    route_weight = route_weight / lax.optimization_barrier(jnp.sum(route_weight, axis=-1, keepdims=True))
    combined = lax.optimization_barrier(jnp.sum(picked.astype(jnp.float32) * route_weight[:, :, None], axis=1))
    return (residual_mid.astype(jnp.float32) + combined).astype(jnp.bfloat16)
```

```python
import functools
import math

import jax
import jax.numpy as jnp
from jax import lax
from jax.experimental import pallas as pl
from jax.experimental.pallas import tpu as pltpu
from jax.sharding import PartitionSpec as P

QH = 32
KVH = 4
HD = 64
WIN = 128
TOP = 4


epsilon = 1e-05
rope_base = 150000.0
glu_slope = 1.702


def shifted(value, axis, steps):
    count = lax.axis_size(axis)
    initial, last = (max(0, -steps), min(count, count - steps))
    return lax.ppermute(value, axis, [(source, source + steps) for source in range(initial, last)])


def norm_scale(values, gain):
    widened = values.astype(jnp.float32)
    mean_sq = jnp.mean(widened * widened, axis=-1, keepdims=True)
    return widened * lax.rsqrt(mean_sq + epsilon) * gain


def rotate(values, positions):
    half_width = values.shape[-1] // 2
    freq_steps = jnp.arange(half_width).astype(jnp.float32)
    inverse = jnp.exp(freq_steps * (-2.0 * math.log(rope_base) / values.shape[-1]))
    angles = positions[:, None] * inverse[None, :]
    cosine = jnp.cos(angles)[:, None, :]
    sine_term = jnp.sin(angles)[:, None, :]
    lower_half = values[..., :half_width]
    second = values[..., half_width:]
    return jnp.concatenate(
        [lower_half * cosine - second * sine_term, second * cosine + lower_half * sine_term],
        axis=-1,
    )


def band_block(queries, key_heads, value_heads, sinks, first_pos):
    count = queries.shape[0]
    groups = QH // KVH
    grouped = queries.reshape(count, KVH, groups, HD)
    scores = jnp.einsum(
        "tkgd,skd->kgts", grouped, key_heads, preferred_element_type=jnp.float32
    ) * (1.0 / math.sqrt(HD))
    query_pos = first_pos + jnp.arange(count)
    key_pos = first_pos - count + jnp.arange(2 * count)
    distance = query_pos[:, None] - key_pos[None, :]
    allowed = (distance >= 0) & (distance < WIN) & (key_pos >= 0)[None, :]
    scores = jnp.where(allowed[None, None, :, :], scores, -jnp.inf)
    sink_logit = sinks.reshape(KVH, groups, 1, 1)
    row_peak = jnp.maximum(jnp.max(scores, axis=-1, keepdims=True), sink_logit)
    raised = jnp.exp(scores - row_peak)
    totals = jnp.sum(raised, axis=-1, keepdims=True) + jnp.exp(sink_logit - row_peak)
    weights = (raised / totals).astype(jnp.bfloat16)
    mixture = jnp.einsum("kgts,skd->tkgd", weights, value_heads, preferred_element_type=jnp.float32)
    return mixture.reshape(count, QH * HD).astype(jnp.bfloat16)


def run_expert(incoming, weight_in, weight_out):
    width = incoming.shape[-1]
    hidden_width = weight_in.shape[1] // 2
    flat_rows = incoming.reshape(-1, width)
    paired = jnp.dot(flat_rows, weight_in, preferred_element_type=jnp.float32)
    gate_part = paired[:, :hidden_width]
    up_part = paired[:, hidden_width:]
    activated = (gate_part * jax.nn.sigmoid(glu_slope * gate_part) * (up_part + 1.0)).astype(
        jnp.bfloat16
    )
    produced = jnp.dot(activated, weight_out, preferred_element_type=jnp.float32).astype(
        jnp.bfloat16
    )
    return produced.reshape(incoming.shape)


LANES = 128


def ring_neighbours(axis, count):
    index = lax.axis_index(axis)
    row, column = index // 2, index % 2
    rows = count // 2
    up = column == 0
    after = jnp.where(up, jnp.where(row < rows - 1, index + 2, index + 1), jnp.where(row > 0, index - 2, index - 1))
    before = jnp.where(up, jnp.where(row > 0, index - 2, index + 1), jnp.where(row < rows - 1, index + 2, index - 1))
    return after, before


def greet(others, axis):
    barrier = pltpu.get_barrier_semaphore()
    for other in others:
        pl.semaphore_signal(barrier, inc=1, device_id={axis: other}, device_id_type=pl.DeviceIdType.MESH)
    pl.semaphore_wait(barrier, len(others))


def moe_kernel(
    count,
    width,
    x_ref,
    residual_ref,
    win_ref,
    wout_ref,
    out_ref,
    rows_in,
    part_out,
    part_in,
    own,
    gather_send,
    gather_recv,
    part_send,
    part_recv,
):
    half = x_ref.shape[0] // 2
    hidden = wout_ref.shape[1]
    me = lax.axis_index("seq")
    targets = ring_neighbours("seq", count)
    greet(targets, "seq")

    def gather_copy(side, step, source):
        return pltpu.make_async_remote_copy(
            src_ref=source,
            dst_ref=rows_in.at[step, side],
            send_sem=gather_send.at[step, side],
            recv_sem=gather_recv.at[step, side],
            device_id={"seq": targets[side]},
            device_id_type=pl.DeviceIdType.MESH,
        )

    def part_copy(side, step):
        return pltpu.make_async_remote_copy(
            src_ref=part_out.at[step, side],
            dst_ref=part_in.at[step, side],
            send_sem=part_send.at[step, side],
            recv_sem=part_recv.at[step, side],
            device_id={"seq": targets[side]},
            device_id_type=pl.DeviceIdType.MESH,
        )

    def own_half(side):
        return x_ref.at[pl.ds(side * half, half), :]

    def expert(block):
        paired = jnp.dot(block[:, :width], win_ref[0], preferred_element_type=jnp.float32)
        gate_part = paired[:, :hidden]
        up_part = paired[:, hidden:]
        activated = gate_part * jax.nn.sigmoid(glu_slope * gate_part) * (up_part + 1.0)
        produced = jnp.dot(
            activated.astype(jnp.bfloat16), wout_ref[0], preferred_element_type=jnp.float32
        )
        tail = block[:, block.shape[1] - LANES :].astype(jnp.float32)
        lane = lax.broadcasted_iota(jnp.int32, tail.shape, 1)
        first = width - (block.shape[1] - LANES)
        mine = (lane == first + me) | (lane == first + count + me)
        weight = jnp.sum(jnp.where(mine, tail, 0.0), axis=1, keepdims=True)
        return produced.astype(jnp.bfloat16).astype(jnp.float32) * weight

    for side in range(2):
        gather_copy(side, 1, own_half(side)).start()
    own[...] = expert(x_ref[...]) + residual_ref[...].astype(jnp.float32)

    def body(step, carry):
        for side in range(2):
            gather_copy(side, step, own_half(side)).wait_recv()

        @pl.when(step < count - 1)
        def _():
            for side in range(2):
                gather_copy(side, step + 1, rows_in.at[step, side]).start()

        both = expert(rows_in[step].reshape(2 * half, rows_in.shape[-1]))

        @pl.when(step > 1)
        def _():
            for side in range(2):
                part_copy(side, step - 1).wait_recv()

        for side in range(2):
            before = part_in[step - 1, side].astype(jnp.float32)
            before = jnp.where(step > 1, before, 0.0)
            part_out[step, side] = (both[side * half : (side + 1) * half] + before).astype(jnp.bfloat16)
            part_copy(side, step).start()
        return carry

    part_in[0] = jnp.zeros(part_in.shape[1:], part_in.dtype)
    lax.fori_loop(1, count, body, 0)
    for side in range(2):
        part_copy(side, count - 1).wait_recv()
        block = pl.ds(side * half, half)
        out_ref[block, :] = (own[block, :] + part_in[count - 1, side].astype(jnp.float32)).astype(out_ref.dtype)

    def drain(step, carry):
        for side in range(2):
            gather_copy(side, step, own_half(side)).wait_send()
            part_copy(side, step).wait_send()
        return carry

    lax.fori_loop(1, count, drain, 0)


def dense_experts(moe_input, residual_mid, route_weight, expert_ids, expert_in, expert_out):
    rows, width = moe_input.shape
    count = lax.axis_size("seq")
    named = expert_ids[:, :, None] == jnp.arange(count)[None, None, :]
    table = jnp.sum(jnp.where(named, route_weight[:, :, None], 0.0), axis=1)
    high = lax.reduce_precision(table, 8, 7)
    low = (table - high).astype(jnp.bfloat16)
    padded = -(-(width + 2 * count) // LANES) * LANES
    filler = jnp.zeros((rows, padded - width - 2 * count), jnp.bfloat16)
    block = jnp.concatenate([moe_input, high.astype(jnp.bfloat16), low, filler], axis=1)
    half = rows // 2
    vmem = pl.BlockSpec(memory_space=pltpu.VMEM)
    return pl.pallas_call(
        functools.partial(moe_kernel, count, width),
        out_shape=jax.ShapeDtypeStruct((rows, width), jnp.bfloat16),
        in_specs=[vmem] * 4,
        out_specs=vmem,
        scratch_shapes=[
            pltpu.VMEM((count, 2, half, padded), jnp.bfloat16),
            pltpu.VMEM((count, 2, half, width), jnp.bfloat16),
            pltpu.VMEM((count, 2, half, width), jnp.bfloat16),
            pltpu.VMEM((rows, width), jnp.float32),
            pltpu.SemaphoreType.DMA((count, 2)),
            pltpu.SemaphoreType.DMA((count, 2)),
            pltpu.SemaphoreType.DMA((count, 2)),
            pltpu.SemaphoreType.DMA((count, 2)),
        ],
        compiler_params=pltpu.CompilerParams(collective_id=0, has_side_effects=True),
        name="moe_ring",
    )(block, residual_mid, expert_in, expert_out)


def local(
    tokens,
    norm_gain,
    qkv_weight,
    sinks,
    out_weight,
    moe_gain,
    expert_in,
    expert_out,
    expert_ids,
    gate_ints,
):
    local_rows = tokens.shape[0]
    width = tokens.shape[1]
    devices = lax.axis_size("seq")
    device_index = lax.axis_index("seq")
    capacity = 2 * local_rows * TOP // devices
    query_cols = QH * HD
    key_cols = KVH * HD
    residual = tokens.astype(jnp.float32)
    normed = norm_scale(tokens, norm_gain).astype(jnp.bfloat16)
    spread = jnp.dot(
        lax.all_gather(normed, "seq", axis=0, tiled=True),
        qkv_weight,
        preferred_element_type=jnp.float32,
    )
    projections = lax.all_to_all(
        spread.astype(jnp.bfloat16), "seq", split_axis=0, concat_axis=1, tiled=True
    ).astype(jnp.float32)
    first_pos = device_index * local_rows
    positions = (first_pos + jnp.arange(local_rows)).astype(jnp.float32)
    queries = rotate(projections[:, :query_cols].reshape(local_rows, QH, HD), positions).astype(
        jnp.bfloat16
    )
    key_heads = rotate(
        projections[:, query_cols : query_cols + key_cols].reshape(local_rows, KVH, HD), positions
    ).astype(jnp.bfloat16)
    value_heads = (
        projections[:, query_cols + key_cols :].reshape(local_rows, KVH, HD).astype(jnp.bfloat16)
    )
    prev_keys, prev_values = shifted((key_heads, value_heads), "seq", 1)
    key_block = jnp.concatenate([prev_keys, key_heads], axis=0)
    value_block = jnp.concatenate([prev_values, value_heads], axis=0)
    attention = band_block(queries, key_block, value_block, sinks, first_pos)
    projected = jnp.dot(
        attention,
        lax.all_gather(out_weight, "seq", axis=0, tiled=True),
        preferred_element_type=jnp.float32,
    )
    residual_mid = (residual + projected).astype(jnp.bfloat16)
    moe_input = norm_scale(residual_mid, moe_gain).astype(jnp.bfloat16)
    route_weight = gate_ints.astype(jnp.float32)
    route_weight = route_weight / jnp.sum(route_weight, axis=-1, keepdims=True)
    tail = width % LANES + 2 * devices
    if capacity >= local_rows and devices % 2 == 0 and tail <= LANES:
        return dense_experts(
            moe_input, residual_mid, route_weight, expert_ids, expert_in, expert_out
        )
    flat_ids = expert_ids.reshape(-1)
    onehot = (flat_ids[:, None] == jnp.arange(devices)[None, :]).astype(jnp.int32)
    before = jnp.cumsum(onehot, axis=0) - onehot
    slot_index = jnp.sum(before * onehot, axis=1)
    target = flat_ids * capacity + slot_index
    matches = target[None, :] == jnp.arange(devices * capacity)[:, None]
    owner_row = jnp.sum(jnp.where(matches, jnp.arange(local_rows * TOP)[None, :], 0), axis=1)
    filled = jnp.any(matches, axis=1)
    gathered = jnp.take(moe_input, owner_row // TOP, axis=0)
    outgoing = jnp.where(filled[:, None], gathered, jnp.zeros_like(gathered)).reshape(
        devices, capacity, width
    )
    arrived = lax.all_to_all(outgoing, "seq", split_axis=0, concat_axis=0, tiled=True)
    returned = lax.all_to_all(
        run_expert(arrived, expert_in[0], expert_out[0]),
        "seq",
        split_axis=0,
        concat_axis=0,
        tiled=True,
    )
    picked = jnp.take(returned.reshape(-1, width), target, axis=0).reshape(local_rows, TOP, width)
    combined = residual_mid.astype(jnp.float32)
    for which in range(TOP):
        combined = combined + route_weight[:, which : which + 1] * picked[:, which].astype(
            jnp.float32
        )
    return combined.astype(jnp.bfloat16)


def solution(mesh):
    return jax.shard_map(
        local,
        mesh=mesh,
        in_specs=(
            P(("batch", "seq"), None),
            P(),
            P(None, "seq"),
            P(),
            P("seq", None),
            P(),
            P("seq", None, None),
            P("seq", None, None),
            P(("batch", "seq"), None),
            P(("batch", "seq"), None),
        ),
        out_specs=P(("batch", "seq"), None),
        check_vma=False,
    )
```

```python
import functools
import math

import jax
import jax.numpy as jnp
from jax import lax
from jax.experimental import pallas as pl
from jax.experimental.pallas import tpu as pltpu
from jax.sharding import PartitionSpec as P

QH = 32
KVH = 4
HD = 64
WIN = 128
TOP = 4


epsilon = 1e-05
rope_base = 150000.0
glu_slope = 1.702


def shifted(value, axis, steps):
    count = lax.axis_size(axis)
    initial, last = (max(0, -steps), min(count, count - steps))
    return lax.ppermute(value, axis, [(source, source + steps) for source in range(initial, last)])


def norm_scale(values, gain):
    widened = values.astype(jnp.float32)
    mean_sq = jnp.mean(widened * widened, axis=-1, keepdims=True)
    return widened * lax.rsqrt(mean_sq + epsilon) * gain


def rotate(values, positions):
    half_width = values.shape[-1] // 2
    freq_steps = jnp.arange(half_width).astype(jnp.float32)
    inverse = jnp.exp(freq_steps * (-2.0 * math.log(rope_base) / values.shape[-1]))
    angles = positions[:, None] * inverse[None, :]
    cosine = jnp.cos(angles)[:, None, :]
    sine_term = jnp.sin(angles)[:, None, :]
    lower_half = values[..., :half_width]
    second = values[..., half_width:]
    return jnp.concatenate(
        [lower_half * cosine - second * sine_term, second * cosine + lower_half * sine_term],
        axis=-1,
    )


def band_block(queries, key_heads, value_heads, sinks, first_pos):
    count = queries.shape[0]
    groups = QH // KVH
    grouped = queries.reshape(count, KVH, groups, HD)
    scores = jnp.einsum(
        "tkgd,skd->kgts", grouped, key_heads, preferred_element_type=jnp.float32
    ) * (1.0 / math.sqrt(HD))
    query_pos = first_pos + jnp.arange(count)
    key_pos = first_pos - count + jnp.arange(2 * count)
    distance = query_pos[:, None] - key_pos[None, :]
    allowed = (distance >= 0) & (distance < WIN) & (key_pos >= 0)[None, :]
    scores = jnp.where(allowed[None, None, :, :], scores, -jnp.inf)
    sink_logit = sinks.reshape(KVH, groups, 1, 1)
    row_peak = jnp.maximum(jnp.max(scores, axis=-1, keepdims=True), sink_logit)
    raised = jnp.exp(scores - row_peak)
    totals = jnp.sum(raised, axis=-1, keepdims=True) + jnp.exp(sink_logit - row_peak)
    weights = (raised / totals).astype(jnp.bfloat16)
    mixture = jnp.einsum("kgts,skd->tkgd", weights, value_heads, preferred_element_type=jnp.float32)
    return mixture.reshape(count, QH * HD).astype(jnp.bfloat16)


def run_expert(incoming, weight_in, weight_out):
    width = incoming.shape[-1]
    hidden_width = weight_in.shape[1] // 2
    flat_rows = incoming.reshape(-1, width)
    paired = jnp.dot(flat_rows, weight_in, preferred_element_type=jnp.float32)
    gate_part = paired[:, :hidden_width]
    up_part = paired[:, hidden_width:]
    activated = (gate_part * jax.nn.sigmoid(glu_slope * gate_part) * (up_part + 1.0)).astype(
        jnp.bfloat16
    )
    produced = jnp.dot(activated, weight_out, preferred_element_type=jnp.float32).astype(
        jnp.bfloat16
    )
    return produced.reshape(incoming.shape)


LANES = 128


def ring_neighbours(axis, count):
    index = lax.axis_index(axis)
    row, column = index // 2, index % 2
    rows = count // 2
    up = column == 0
    after = jnp.where(up, jnp.where(row < rows - 1, index + 2, index + 1), jnp.where(row > 0, index - 2, index - 1))
    before = jnp.where(up, jnp.where(row > 0, index - 2, index + 1), jnp.where(row < rows - 1, index + 2, index - 1))
    return after, before


def greet(others, axis, more=()):
    barrier = pltpu.get_barrier_semaphore()
    devices = [{axis: other} for other in others] + list(more)
    for device in devices:
        pl.semaphore_signal(barrier, inc=1, device_id=device, device_id_type=pl.DeviceIdType.MESH)
    pl.semaphore_wait(barrier, len(devices))


def moe_kernel(
    count,
    width,
    x_ref,
    residual_ref,
    win_ref,
    wout_ref,
    out_ref,
    rows_in,
    part_out,
    part_in,
    own,
    gather_send,
    gather_recv,
    part_send,
    part_recv,
):
    half = x_ref.shape[0] // 2
    hidden = wout_ref.shape[1]
    me = lax.axis_index("seq")
    targets = ring_neighbours("seq", count)
    greet(targets, "seq")

    def gather_copy(side, step, source):
        return pltpu.make_async_remote_copy(
            src_ref=source,
            dst_ref=rows_in.at[step, side],
            send_sem=gather_send.at[step, side],
            recv_sem=gather_recv.at[step, side],
            device_id={"seq": targets[side]},
            device_id_type=pl.DeviceIdType.MESH,
        )

    def part_copy(side, step):
        return pltpu.make_async_remote_copy(
            src_ref=part_out.at[step, side],
            dst_ref=part_in.at[step, side],
            send_sem=part_send.at[step, side],
            recv_sem=part_recv.at[step, side],
            device_id={"seq": targets[side]},
            device_id_type=pl.DeviceIdType.MESH,
        )

    def own_half(side):
        return x_ref.at[pl.ds(side * half, half), :]

    def expert(block):
        paired = jnp.dot(block[:, :width], win_ref[0], preferred_element_type=jnp.float32)
        gate_part = paired[:, :hidden]
        up_part = paired[:, hidden:]
        activated = gate_part * jax.nn.sigmoid(glu_slope * gate_part) * (up_part + 1.0)
        produced = jnp.dot(
            activated.astype(jnp.bfloat16), wout_ref[0], preferred_element_type=jnp.float32
        )
        tail = block[:, block.shape[1] - LANES :].astype(jnp.float32)
        lane = lax.broadcasted_iota(jnp.int32, tail.shape, 1)
        first = width - (block.shape[1] - LANES)
        mine = (lane == first + me) | (lane == first + count + me)
        weight = jnp.sum(jnp.where(mine, tail, 0.0), axis=1, keepdims=True)
        return produced.astype(jnp.bfloat16).astype(jnp.float32) * weight

    for side in range(2):
        gather_copy(side, 1, own_half(side)).start()
    own[...] = expert(x_ref[...]) + residual_ref[...].astype(jnp.float32)

    def body(step, carry):
        for side in range(2):
            gather_copy(side, step, own_half(side)).wait_recv()

        @pl.when(step < count - 1)
        def _():
            for side in range(2):
                gather_copy(side, step + 1, rows_in.at[step, side]).start()

        both = expert(rows_in[step].reshape(2 * half, rows_in.shape[-1]))

        @pl.when(step > 1)
        def _():
            for side in range(2):
                part_copy(side, step - 1).wait_recv()

        for side in range(2):
            before = part_in[step - 1, side].astype(jnp.float32)
            before = jnp.where(step > 1, before, 0.0)
            part_out[step, side] = (both[side * half : (side + 1) * half] + before).astype(jnp.bfloat16)
            part_copy(side, step).start()
        return carry

    part_in[0] = jnp.zeros(part_in.shape[1:], part_in.dtype)
    lax.fori_loop(1, count, body, 0)
    for side in range(2):
        part_copy(side, count - 1).wait_recv()
        block = pl.ds(side * half, half)
        out_ref[block, :] = (own[block, :] + part_in[count - 1, side].astype(jnp.float32)).astype(out_ref.dtype)

    def drain(step, carry):
        for side in range(2):
            gather_copy(side, step, own_half(side)).wait_send()
            part_copy(side, step).wait_send()
        return carry

    lax.fori_loop(1, count, drain, 0)


def dense_experts(moe_input, residual_mid, route_weight, expert_ids, expert_in, expert_out):
    rows, width = moe_input.shape
    count = lax.axis_size("seq")
    named = expert_ids[:, :, None] == jnp.arange(count)[None, None, :]
    table = jnp.sum(jnp.where(named, route_weight[:, :, None], 0.0), axis=1)
    high = lax.reduce_precision(table, 8, 7)
    low = (table - high).astype(jnp.bfloat16)
    padded = -(-(width + 2 * count) // LANES) * LANES
    filler = jnp.zeros((rows, padded - width - 2 * count), jnp.bfloat16)
    block = jnp.concatenate([moe_input, high.astype(jnp.bfloat16), low, filler], axis=1)
    half = rows // 2
    vmem = pl.BlockSpec(memory_space=pltpu.VMEM)
    return pl.pallas_call(
        functools.partial(moe_kernel, count, width),
        out_shape=jax.ShapeDtypeStruct((rows, width), jnp.bfloat16),
        in_specs=[vmem] * 4,
        out_specs=vmem,
        scratch_shapes=[
            pltpu.VMEM((count, 2, half, padded), jnp.bfloat16),
            pltpu.VMEM((count, 2, half, width), jnp.bfloat16),
            pltpu.VMEM((count, 2, half, width), jnp.bfloat16),
            pltpu.VMEM((rows, width), jnp.float32),
            pltpu.SemaphoreType.DMA((count, 2)),
            pltpu.SemaphoreType.DMA((count, 2)),
            pltpu.SemaphoreType.DMA((count, 2)),
            pltpu.SemaphoreType.DMA((count, 2)),
        ],
        compiler_params=pltpu.CompilerParams(collective_id=0, has_side_effects=True),
        name="moe_ring",
    )(block, residual_mid, expert_in, expert_out)


def weights_kernel(
    count,
    x_ref,
    qkv_ref,
    out_weight_ref,
    spread_ref,
    out_all_ref,
    qkv_all,
    ring_send,
    ring_recv,
    across_send,
    across_recv,
    core_send,
    core_recv,
):
    me = lax.axis_index("seq")
    seat = lax.axis_index("batch")
    core, side = seat % 2, seat // 2
    partner, across = seat + 1 - 2 * core, seat + 2 - 4 * side
    rows = count // 2
    place = jnp.where(me % 2 == 0, me // 2, count - 1 - me // 2)
    targets = ring_neighbours("seq", count)
    greet(targets, "seq", ({"batch": partner}, {"batch": across}))
    shards = (qkv_ref, out_weight_ref)
    gathered = (qkv_all, out_all_ref)

    def shard_at(position):
        position = lax.rem(position + count, count)
        return jnp.where(position < rows, 2 * position, 2 * (count - 1 - position) + 1)

    def piece(which, third):
        size = shards[which].shape[0] // 6
        return pl.ds(pl.multiple_of((third * 2 + core) * size, 16), size)

    def remote(source, target, send, recv, device):
        return pltpu.make_async_remote_copy(
            src_ref=source,
            dst_ref=target,
            send_sem=send,
            recv_sem=recv,
            device_id=device,
            device_id_type=pl.DeviceIdType.MESH,
        )

    def ring_copy(way, step, which, first=False):
        shard = shard_at(place + (1 - 2 * way) * (1 - step))
        span = piece(which, side + way)
        target = gathered[which].at[shard, span]
        source = shards[which].at[span] if first else target
        sems = ring_send.at[way, step, which], ring_recv.at[way, step, which]
        return remote(source, target, *sems, {"seq": targets[way]})

    def across_copy(step, which):
        shard = shard_at(place + (2 * side - 1) * step)
        target = gathered[which].at[shard, piece(which, 2 * side)]
        sems = across_send.at[step, which], across_recv.at[step, which]
        return remote(target, target, *sems, {"batch": across})

    def core_copy(kind, step, which):
        third = (side, side + 1, 2 * (1 - side))[kind]
        offset = (-step, step, (1 - 2 * side) * step)[kind]
        target = gathered[which].at[shard_at(place + offset), piece(which, third)]
        sems = core_send.at[kind, step, which], core_recv.at[kind, step, which]
        return remote(target, target, *sems, {"batch": partner})

    for which in range(2):
        for way in range(2):
            ring_copy(way, 1, which, True).start()
    for which in range(2):
        gathered[which][me] = shards[which][...]

    def body(step, carry):
        for which in range(2):
            for way in range(2):
                ring_copy(way, step, which).wait_recv()

                @pl.when(step < count - 1)
                def _():
                    ring_copy(way, step + 1, which).start()

            across_copy(step, which).start()
            for way in range(2):
                core_copy(way, step, which).start()

            @pl.when(step > 1)
            def _():
                across_copy(step - 1, which).wait_recv()
                core_copy(2, step - 1, which).start()

        return carry

    lax.fori_loop(1, count, body, 0)
    for which in range(2):
        across_copy(count - 1, which).wait_recv()
        core_copy(2, count - 1, which).start()

    def arrived(which):
        def wait(step, carry):
            for kind in range(3):
                core_copy(kind, step, which).wait_recv()
            return carry

        lax.fori_loop(1, count, wait, 0)

    arrived(0)

    def project(shard, carry):
        spread_ref[shard] = jnp.dot(x_ref[...], qkv_all[shard], preferred_element_type=jnp.float32)
        return carry

    lax.fori_loop(0, count, project, 0)
    arrived(1)

    def drain(step, carry):
        for which in range(2):
            for way in range(2):
                ring_copy(way, step, which).wait_send()
            across_copy(step, which).wait_send()
            for kind in range(3):
                core_copy(kind, step, which).wait_send()
        return carry

    lax.fori_loop(1, count, drain, 0)


def gather_weights(normed, qkv_weight, out_weight):
    count = lax.axis_size("seq")
    depth = out_weight.shape[0]
    padded = -(-depth // 96) * 96
    out_weight = jnp.pad(out_weight, ((0, padded - depth), (0, 0)))
    vmem = pl.BlockSpec(memory_space=pltpu.VMEM)
    shape = (normed.shape[0], qkv_weight.shape[1])
    dma = pltpu.SemaphoreType.DMA
    spread, out_all = pl.pallas_call(
        functools.partial(weights_kernel, count),
        out_shape=(
            jax.ShapeDtypeStruct((count, *shape), jnp.float32),
            jax.ShapeDtypeStruct((count, *out_weight.shape), jnp.bfloat16),
        ),
        in_specs=[vmem] * 3,
        out_specs=(vmem, vmem),
        scratch_shapes=[
            pltpu.VMEM((count, *qkv_weight.shape), jnp.bfloat16),
            dma((2, count, 2)),
            dma((2, count, 2)),
            dma((count, 2)),
            dma((count, 2)),
            dma((3, count, 2)),
            dma((3, count, 2)),
        ],
        compiler_params=pltpu.CompilerParams(collective_id=1, has_side_effects=True),
        name="weights_ring",
    )(normed, qkv_weight, out_weight)
    return spread, out_all.reshape(count * padded, -1), padded


def local(
    tokens,
    norm_gain,
    qkv_weight,
    sinks,
    out_weight,
    moe_gain,
    expert_in,
    expert_out,
    expert_ids,
    gate_ints,
):
    local_rows = tokens.shape[0]
    width = tokens.shape[1]
    devices = lax.axis_size("seq")
    device_index = lax.axis_index("seq")
    capacity = 2 * local_rows * TOP // devices
    query_cols = QH * HD
    key_cols = KVH * HD
    residual = tokens.astype(jnp.float32)
    normed = norm_scale(tokens, norm_gain).astype(jnp.bfloat16)
    tail = width % LANES + 2 * devices
    dense = capacity >= local_rows and devices % 2 == 0 and tail <= LANES
    shared = dense and lax.axis_size("batch") == 4 and width % 96 == 0
    if shared:
        spread, out_all, padded = gather_weights(normed, qkv_weight, out_weight)
        projections = spread.transpose(1, 0, 2).reshape(local_rows, -1)
    else:
        spread = jnp.dot(
            lax.all_gather(normed, "seq", axis=0, tiled=True),
            qkv_weight,
            preferred_element_type=jnp.float32,
        )
        projections = lax.all_to_all(
            spread.astype(jnp.bfloat16), "seq", split_axis=0, concat_axis=1, tiled=True
        ).astype(jnp.float32)
    first_pos = device_index * local_rows
    positions = (first_pos + jnp.arange(local_rows)).astype(jnp.float32)
    queries = rotate(projections[:, :query_cols].reshape(local_rows, QH, HD), positions).astype(
        jnp.bfloat16
    )
    key_heads = rotate(
        projections[:, query_cols : query_cols + key_cols].reshape(local_rows, KVH, HD), positions
    ).astype(jnp.bfloat16)
    value_heads = (
        projections[:, query_cols + key_cols :].reshape(local_rows, KVH, HD).astype(jnp.bfloat16)
    )
    prev_keys, prev_values = shifted((key_heads, value_heads), "seq", 1)
    key_block = jnp.concatenate([prev_keys, key_heads], axis=0)
    value_block = jnp.concatenate([prev_values, value_heads], axis=0)
    attention = band_block(queries, key_block, value_block, sinks, first_pos)
    if shared:
        depth = query_cols // devices
        spaced = jnp.pad(
            attention.reshape(local_rows, devices, depth), ((0, 0), (0, 0), (0, padded - depth))
        ).reshape(local_rows, devices * padded)
        projected = jnp.dot(spaced, out_all, preferred_element_type=jnp.float32)
    else:
        projected = jnp.dot(
            attention,
            lax.all_gather(out_weight, "seq", axis=0, tiled=True),
            preferred_element_type=jnp.float32,
        )
    residual_mid = (residual + projected).astype(jnp.bfloat16)
    moe_input = norm_scale(residual_mid, moe_gain).astype(jnp.bfloat16)
    route_weight = gate_ints.astype(jnp.float32)
    route_weight = route_weight / jnp.sum(route_weight, axis=-1, keepdims=True)
    if dense:
        return dense_experts(
            moe_input, residual_mid, route_weight, expert_ids, expert_in, expert_out
        )
    flat_ids = expert_ids.reshape(-1)
    onehot = (flat_ids[:, None] == jnp.arange(devices)[None, :]).astype(jnp.int32)
    before = jnp.cumsum(onehot, axis=0) - onehot
    slot_index = jnp.sum(before * onehot, axis=1)
    target = flat_ids * capacity + slot_index
    matches = target[None, :] == jnp.arange(devices * capacity)[:, None]
    owner_row = jnp.sum(jnp.where(matches, jnp.arange(local_rows * TOP)[None, :], 0), axis=1)
    filled = jnp.any(matches, axis=1)
    gathered = jnp.take(moe_input, owner_row // TOP, axis=0)
    outgoing = jnp.where(filled[:, None], gathered, jnp.zeros_like(gathered)).reshape(
        devices, capacity, width
    )
    arrived = lax.all_to_all(outgoing, "seq", split_axis=0, concat_axis=0, tiled=True)
    returned = lax.all_to_all(
        run_expert(arrived, expert_in[0], expert_out[0]),
        "seq",
        split_axis=0,
        concat_axis=0,
        tiled=True,
    )
    picked = jnp.take(returned.reshape(-1, width), target, axis=0).reshape(local_rows, TOP, width)
    combined = residual_mid.astype(jnp.float32)
    for which in range(TOP):
        combined = combined + route_weight[:, which : which + 1] * picked[:, which].astype(
            jnp.float32
        )
    return combined.astype(jnp.bfloat16)


def solution(mesh):
    return jax.shard_map(
        local,
        mesh=mesh,
        in_specs=(
            P(("batch", "seq"), None),
            P(),
            P(None, "seq"),
            P(),
            P("seq", None),
            P(),
            P("seq", None, None),
            P("seq", None, None),
            P(("batch", "seq"), None),
            P(("batch", "seq"), None),
        ),
        out_specs=P(("batch", "seq"), None),
        check_vma=False,
    )
```
